16 devices in a mesh: tp: 2 (over y, z), cp: 8 (over x, core).
Axes of the slice: x: 4, y: 2, z: 1, core: 2. Of those that a mesh axis runs over, the one named last changes fastest.
The devices are a block of a 4x4x8 slice.
Arguments:
- query: bfloat16 [32, 128, 14, 128], P(None, 'cp', 'tp'), parts along dimension 2
- out_act: bfloat16 [32, 128, 14, 128], P(None, 'cp', 'tp'), parts along dimension 2
- out_grad: bfloat16 [32, 128, 14, 128], P(None, 'cp', 'tp'), parts along dimension 2
- row_lse: float32 [32, 128, 14], P(None, 'cp', 'tp'), parts along dimension 2
- key_act: bfloat16 [8192, 2, 128], P('cp', 'tp'), parts along dimension 1
- value_act: bfloat16 [8192, 2, 128], P('cp', 'tp'), parts along dimension 1
- doc_ids: int32 [8192], replicated
Outputs:
- output 1: bfloat16 [32, 128, 14, 128], P(None, 'cp', 'tp'), parts along dimension 2
- output 2: float32 [8192, 2, 128], P('cp', 'tp'), parts along dimension 1
- output 3: float32 [8192, 2, 128], P('cp', 'tp'), parts along dimension 1
There are 2 independent parts. The reference program is written for one: setup_inputs(seed, part) draws one part's arguments, and reference() takes and returns one part's arrays. A program takes and returns all parts, laid end to end along the dimension named above; an argument that names none is the same for every part.
All inputs are finite; a program needn't handle non-finite values.
Results may differ from the reference program's by a relative error of at most 0.001.
Values are sent between devices in bfloat16 or wider.
A program may use at most 768 MiB of HBM per device.

```python
import jax
import jax.numpy as jnp
from jax import lax

SLICES = 32
SUB_LEN = 128
PRE_LEN = 4096
Q_HEADS = 7
KV_HEADS = 1
HEAD_DIM = 128
SPLITS = 8

PREFIX = PRE_LEN + SLICES * SUB_LEN
GROUP_SIZE = Q_HEADS // KV_HEADS
BLOCK_LEN = SUB_LEN // SPLITS
SCORE_SCALE = HEAD_DIM ** -0.5
GRAD_SCALE = (PREFIX // 8) ** 0.5
DOC_MEAN = PREFIX // 8


def masked_scores(q_blk, key_act, doc_ids, first_pos):
    block_len = q_blk.shape[0]
    scores = jnp.einsum('qhgd,khd->qhgk', q_blk.astype(jnp.float32), key_act.astype(jnp.float32)) * SCORE_SCALE
    q_pos = first_pos + jnp.arange(block_len)
    k_pos = jnp.arange(key_act.shape[0])
    q_doc = lax.dynamic_slice(doc_ids, (first_pos,), (block_len,))
    allowed = (k_pos[None, :] <= q_pos[:, None]) & (doc_ids[None, :] == q_doc[:, None])
    return scores, allowed[:, None, None, :]


def forward_lse(query, key_act, doc_ids):
    n_blocks = SLICES * SPLITS
    q_blocks = query.reshape(n_blocks, BLOCK_LEN, KV_HEADS, GROUP_SIZE, HEAD_DIM)
    firsts = PRE_LEN + jnp.arange(n_blocks) * BLOCK_LEN

    def block_lse(xs_blk):
        q_blk, first_pos = xs_blk
        scores, allowed = masked_scores(q_blk, key_act, doc_ids, first_pos)
        return jax.nn.logsumexp(jnp.where(allowed, scores, -1e30), axis=-1)

    return lax.map(block_lse, (q_blocks, firsts)).reshape(SLICES, SUB_LEN, Q_HEADS)


def setup_inputs(seed: int = 0, part: int = 0) -> dict:
    root_key = jax.random.key(seed)
    part_keys = jax.random.split(jax.random.fold_in(root_key, part), 5)
    doc_key = jax.random.key(seed + 17)
    starts = (jax.random.randint(doc_key, (PREFIX,), 0, DOC_MEAN) == 0) & (jnp.arange(PREFIX) > 0)
    doc_ids = jnp.cumsum(starts.astype(jnp.int32)).astype(jnp.int32)
    q_shape = (SLICES, SUB_LEN, Q_HEADS, HEAD_DIM)
    query = jax.random.normal(part_keys[0], q_shape, jnp.float32).astype(jnp.bfloat16)
    key_act = jax.random.normal(part_keys[1], (PREFIX, KV_HEADS, HEAD_DIM), jnp.float32).astype(jnp.bfloat16)
    value_act = jax.random.normal(part_keys[2], (PREFIX, KV_HEADS, HEAD_DIM), jnp.float32).astype(jnp.bfloat16)
    grad_dir = jax.random.normal(part_keys[3], q_shape, jnp.float32)
    out_noise = jax.random.normal(part_keys[4], q_shape, jnp.float32)
    out_grad = (GRAD_SCALE * grad_dir).astype(jnp.bfloat16)
    out_act = (0.125 * (grad_dir + out_noise)).astype(jnp.bfloat16)
    row_lse = forward_lse(query, key_act, doc_ids)
    return {'query': query, 'out_act': out_act, 'out_grad': out_grad, 'row_lse': row_lse, 'key_act': key_act, 'value_act': value_act, 'doc_ids': doc_ids}


def reference(query, out_act, out_grad, row_lse, key_act, value_act, doc_ids):
    n_blocks = SLICES * SPLITS
    blk_shape = (n_blocks, BLOCK_LEN, KV_HEADS, GROUP_SIZE, HEAD_DIM)
    key_f32 = key_act.astype(jnp.float32)
    value_f32 = value_act.astype(jnp.float32)
    xs_all = (query.reshape(blk_shape), out_act.reshape(blk_shape), out_grad.reshape(blk_shape), row_lse.reshape(n_blocks, BLOCK_LEN, KV_HEADS, GROUP_SIZE), PRE_LEN + jnp.arange(n_blocks) * BLOCK_LEN)

    def block_step(carry_in, xs_blk):
        dk_acc, dv_acc = carry_in
        q_blk, o_blk, do_blk, lse_blk, first_pos = xs_blk
        scores, allowed = masked_scores(q_blk, key_act, doc_ids, first_pos)
        p_full = jnp.where(allowed, jnp.exp(scores - lse_blk[..., None]), 0.0)
        p_half = p_full.astype(jnp.bfloat16).astype(jnp.float32)
        grad_f32 = do_blk.astype(jnp.float32)
        row_delta = jnp.sum(grad_f32 * o_blk.astype(jnp.float32), axis=-1)
        dv_acc = dv_acc + jnp.einsum('qhgk,qhgd->khd', p_half, grad_f32)
        d_prob = jnp.einsum('qhgd,khd->qhgk', grad_f32, value_f32)
        d_score = (p_full * (d_prob - row_delta[..., None])).astype(jnp.bfloat16).astype(jnp.float32)
        dq_blk = (jnp.einsum('qhgk,khd->qhgd', d_score, key_f32) * SCORE_SCALE).astype(jnp.bfloat16)
        dk_acc = dk_acc + jnp.einsum('qhgk,qhgd->khd', d_score, q_blk.astype(jnp.float32)) * SCORE_SCALE
        return (dk_acc, dv_acc), dq_blk

    zero_acc = jnp.zeros((PREFIX, KV_HEADS, HEAD_DIM), jnp.float32)
    (d_key, d_value), dq_blocks = lax.scan(block_step, (zero_acc, zero_acc), xs_all)
    return dq_blocks.reshape(SLICES, SUB_LEN, Q_HEADS, HEAD_DIM), d_key, d_value
```

```python
import functools

import jax
import jax.numpy as jnp
from jax import lax
from jax.experimental import pallas as pl
from jax.experimental.pallas import tpu as pltpu
from jax.sharding import PartitionSpec as P

LOG2E = 1.4426950408889634
KEY_BLOCK = 256
SUBS_PER_TILE = 2


def grad_kernel(bounds_ref, q_ref, do_ref, stats_ref, kv_ref, kdoc_ref, dkv_ref, dq_out_ref,
                s_buf, dp_buf, dq_acc, *, n_tiles, n_kb, first_kb, kb_per_shard, tile_rows, tile_span, scale):
    kb_len = KEY_BLOCK

    def first_tile(kb):
        return jnp.maximum(kb * kb_len // tile_span - first_kb * kb_len // tile_span, 0)

    dkv_ref[...] = jnp.zeros_like(dkv_ref)
    dq_acc[...] = jnp.zeros_like(dq_acc)

    def count(kb, carry):
        total, start = carry
        n_here = jnp.maximum(bounds_ref[kb] - first_tile(kb), 0)
        start = jnp.where((n_here > 0) & (start < 0), kb, start)
        return total + n_here, start

    n_steps, kb0 = lax.fori_loop(0, n_kb, count, (jnp.int32(0), jnp.int32(-1)))

    def key_slice(kb):
        return kb // kb_per_shard, pl.ds(pl.multiple_of(lax.rem(kb, kb_per_shard) * kb_len, kb_len), kb_len)

    def row_slice(qt):
        return pl.ds(pl.multiple_of(qt * tile_rows, tile_rows), tile_rows)

    def score(kb, qt, slot):
        shard, keys = key_slice(kb)
        rows = row_slice(qt)
        dims = (((1,), (1,)), ((), ()))
        s_buf[slot] = lax.dot_general(q_ref[rows, :], kv_ref[shard, 0, keys, :], dims, preferred_element_type=jnp.float32)
        dp_buf[slot] = lax.dot_general(do_ref[rows, :], kv_ref[shard, 1, keys, :], dims, preferred_element_type=jnp.float32)

    def advance(kb, qt):
        last = qt + 1 >= bounds_ref[kb]
        kb_next = jnp.where(last, jnp.minimum(kb + 1, n_kb - 1), kb)
        qt_next = jnp.where(last, first_tile(kb_next), qt + 1)
        return kb_next, jnp.minimum(qt_next, n_tiles - 1)

    qt0 = first_tile(kb0)
    score(kb0, qt0, 0)

    def step(i, carry):
        kb, qt = carry
        slot = lax.rem(i, 2)
        kb_next, qt_next = advance(kb, qt)
        rows = row_slice(qt)
        shard, keys = key_slice(kb)
        stats = stats_ref[rows, :]
        s_now = s_buf[slot]
        dp_now = dp_buf[slot]
        score(kb_next, qt_next, 1 - slot)
        p_full = jnp.exp2(s_now * (scale * LOG2E) - stats[:, 0:1])
        key_pos = (kb * kb_len + lax.broadcasted_iota(jnp.int32, (1, kb_len), 1)).astype(jnp.float32)
        allowed = (kdoc_ref[kb] == stats[:, 2:3]) & (key_pos <= stats[:, 3:4])
        p_full = jnp.where(allowed, p_full, 0.0)
        ds = (p_full * (dp_now - stats[:, 1:2])).astype(jnp.bfloat16)
        p_half = p_full.astype(jnp.bfloat16)
        tdims = (((0,), (0,)), ((), ()))
        dkv_ref[kb, 1] += lax.dot_general(do_ref[rows, :], p_half, tdims, preferred_element_type=jnp.float32)
        dkv_ref[kb, 0] += lax.dot_general(q_ref[rows, :], ds, tdims, preferred_element_type=jnp.float32)
        dq_acc[rows, :] += jnp.dot(ds, kv_ref[shard, 0, keys, :], preferred_element_type=jnp.float32)
        return kb_next, qt_next

    lax.fori_loop(0, n_steps, step, (kb0, qt0))
    dq_out_ref[...] = (dq_acc[...] * scale).astype(jnp.bfloat16)


def solution(mesh):
    cp_size = mesh.shape['cp']
    q_spec = P(None, 'cp', 'tp', None)
    lse_spec = P(None, 'cp', 'tp')
    kv_spec = P('cp', 'tp', None)

    def local_backward(query, out_act, out_grad, row_lse, key_act, value_act, doc_ids):
        n_sub, local_len, n_heads, head_dim = query.shape
        keys_local = key_act.shape[0]
        sub_len = local_len * cp_size
        n_keys = keys_local * cp_size
        sub_start = n_keys - n_sub * sub_len
        scale = head_dim ** -0.5
        n_rows = n_sub * local_len * n_heads
        tile_rows = SUBS_PER_TILE * local_len * n_heads
        tile_span = SUBS_PER_TILE * sub_len
        n_tiles = n_sub // SUBS_PER_TILE
        n_kb = n_keys // KEY_BLOCK
        me = lax.axis_index('cp')

        kv_local = jnp.stack([key_act[:, 0], value_act[:, 0]])[None]
        kv_all = lax.all_gather(kv_local, 'cp', axis=0, tiled=True)

        q_rows = query.reshape(n_rows, head_dim)
        do_rows = out_grad.reshape(n_rows, head_dim)
        delta = jnp.sum(out_grad.astype(jnp.float32) * out_act.astype(jnp.float32), axis=-1)
        doc_f = doc_ids.astype(jnp.float32)
        q_pos = sub_start + jnp.arange(n_sub)[:, None] * sub_len + me * local_len + jnp.arange(local_len)[None, :]
        q_doc = lax.dynamic_slice(doc_f[sub_start:].reshape(n_sub, sub_len), (0, me * local_len), (n_sub, local_len))
        per_tok = (n_sub, local_len, n_heads)
        stats = jnp.stack([row_lse * LOG2E, delta,
                           jnp.broadcast_to(q_doc[..., None], per_tok),
                           jnp.broadcast_to(q_pos[..., None].astype(jnp.float32), per_tok)], axis=-1).reshape(n_rows, 4)
        last_doc = doc_ids[KEY_BLOCK - 1::KEY_BLOCK]
        last_pos = jnp.sum((doc_ids[None, :] <= last_doc[:, None]).astype(jnp.int32), axis=1) - 1
        bounds = jnp.where(last_pos >= sub_start, (last_pos - sub_start) // tile_span + 1, 0)

        body = functools.partial(grad_kernel, n_tiles=n_tiles, n_kb=n_kb, first_kb=sub_start // KEY_BLOCK,
                                 kb_per_shard=keys_local // KEY_BLOCK, tile_rows=tile_rows, tile_span=tile_span, scale=scale)
        vmem = pl.BlockSpec(memory_space=pltpu.VMEM)
        dkv, dq = pl.pallas_call(
            body,
            out_shape=(jax.ShapeDtypeStruct((n_kb, 2, head_dim, KEY_BLOCK), jnp.float32),
                       jax.ShapeDtypeStruct((n_rows, head_dim), jnp.bfloat16)),
            in_specs=[pl.BlockSpec(memory_space=pltpu.SMEM)] + [vmem] * 5,
            out_specs=(vmem, vmem),
            scratch_shapes=[pltpu.VMEM((2, tile_rows, KEY_BLOCK), jnp.float32),
                            pltpu.VMEM((2, tile_rows, KEY_BLOCK), jnp.float32),
                            pltpu.VMEM((n_rows, head_dim), jnp.float32)],
            compiler_params=pltpu.CompilerParams(vmem_limit_bytes=60 << 20),
            name='attn_grad',
        )(bounds, q_rows, do_rows, stats, kv_all, doc_f.reshape(n_kb, 1, KEY_BLOCK))

        dkv = lax.psum_scatter(dkv, 'cp', scatter_dimension=0, tiled=True)
        dkv = dkv.transpose(1, 0, 3, 2).reshape(2, keys_local, 1, head_dim)
        return dq.reshape(query.shape), dkv[0] * scale, dkv[1]

    return jax.shard_map(local_backward, mesh=mesh, in_specs=(q_spec, q_spec, q_spec, lse_spec, kv_spec, kv_spec, P()), out_specs=(q_spec, kv_spec, kv_spec), check_vma=False)
```
